32 devices in a mesh: groups: 2 (over y), rows: 4 (over z), keys: 2 (over x), heads: 2 (over core).
Axes of the slice: x: 2, y: 2, z: 4, core: 2. Of those that a mesh axis runs over, the one named last changes fastest.
Arguments:
- pair: bfloat16 [1024, 512, 128], P(('groups', 'rows'), 'keys'), parts along dimension 0, may hold values from -6 to 6
- seq_length: int32 [2], P('groups'), parts along dimension 0, may hold values from 257 to 512
- tile_counts: int32 [1024, 4], P(('groups', 'rows')), parts along dimension 0, may hold values from 0 to 128, as said below
- ln_gain: float32 [128], replicated, may hold values from 0.5 to 1.5
- w_query: bfloat16 [128, 128], P(None, 'heads'), may hold values from -8 to 8
- w_key: bfloat16 [128, 128], P(None, 'heads'), may hold values from -0.5 to 0.5
- w_value: bfloat16 [128, 128], P(None, 'heads'), may hold values from -0.5 to 0.5
- w_gate: bfloat16 [128, 128], P(None, 'heads'), may hold values from -0.5 to 0.5
- w_bias: bfloat16 [128, 4], P(None, 'heads'), may hold values from -1.5 to 1.5
- w_out: bfloat16 [128, 128], replicated, may hold values from -2 to 2
Outputs:
- update: bfloat16 [1024, 512, 128], P(('groups', 'rows'), ('keys', 'heads')), parts along dimension 0
The draws below stay inside these ranges and needn't reach their ends.
There are 2 independent parts, one for each index of `groups`. The reference program is written for one: setup_inputs(seed, part) draws one part's arguments, and reference() takes and returns one part's arrays. A program takes and returns all parts, laid end to end along the dimension named above; an argument that names none is the same for every part. Nothing has to cross between parts.
Inputs may be any that keep to these rules, and one draw needn't show every extreme that they name: `tile_counts`: for each row and each tile of 128 keys, how many of the tile's leading keys are valid; some rows have no valid key at all.
All inputs are finite; a program needn't handle non-finite values.
Results may differ from the reference program's by a relative error of at most 0.03.
The reference program's roundings to bfloat16 on the way count: a program that leaves them out, or rounds other values in their place, can miss the bound.
Values may be sent and summed in bfloat16 or wider, within the bound.
A program may use at most 192 MiB of HBM per device.

```python
import jax
import jax.numpy as jnp
from jax import lax

C = 128
HEADS = 4
HEAD_DIM = 32
TILE = 128
L = 512


def draw_tile_counts(key, part):
    first, second = jax.random.split(jax.random.fold_in(key, 11))
    counts = jax.random.randint(first, (L, L // TILE), 0, TILE + 1)
    keeper = jax.random.randint(second, (L, 1), 0, 8) > 0
    return jnp.where(keeper, counts, 0).astype(jnp.int32)


def draw_w_query(key, part):
    inner = jax.random.fold_in(key, 23)
    drawn = jnp.clip(jax.random.normal(inner, (C, HEADS * HEAD_DIM), jnp.float32), -4.0, 4.0) * C ** (-0.5)
    return drawn.astype(jnp.bfloat16)


def block_levels(stream_key, extent, cuts, least, top_value):
    def one(position, blocks):
        heights = jax.random.uniform(jax.random.fold_in(jax.random.fold_in(stream_key, 6), position), (blocks,), jnp.float32, least / len(cuts), top_value / len(cuts))
        return jnp.repeat(jnp.exp(heights), extent[position] // blocks).reshape((-1,) + (1,) * (len(extent) - position - 1))

    level = one(*cuts[0])
    for cut in cuts[1:]:
        level = level * one(*cut)
    return level


def centred(rng, extent, deviation, reach, cuts=(), kind=jnp.bfloat16):
    values = deviation * jax.random.normal(rng, extent, jnp.float32)
    if cuts:
        values = values * block_levels(rng, extent, cuts, -0.22, 0.18)
    return jnp.clip(values, -reach, reach).astype(kind)


def setup_inputs(seed: int = 0, part: int = 0) -> dict:
    streams_of = jax.random.split(jax.random.key(seed), 11)
    part_splits = jax.random.split(jax.random.fold_in(streams_of[10], part), 11)
    pair = centred(part_splits[0], (L, L, C), 1.0, 6.0, ((0, 4), (1, 2)))
    seq_length = jax.random.randint(part_splits[1], (1,), L // 2 + 1, L + 1).astype(jnp.int32)
    tile_counts = draw_tile_counts(jax.random.fold_in(jax.random.fold_in(streams_of[10], part), 71), part)
    ln_gain = jnp.clip(1.0 + 0.1 * jax.random.normal(streams_of[3], (C,), jnp.float32), 0.5, 1.5)
    w_query = draw_w_query(jax.random.fold_in(streams_of[10], 71), part)
    w_key = centred(streams_of[5], (C, HEADS * HEAD_DIM), C ** -0.5, 0.5, ((1, 2),))
    w_value = centred(streams_of[6], (C, HEADS * HEAD_DIM), C ** -0.5, 0.5, ((1, 2),))
    w_gate = centred(streams_of[7], (C, HEADS * HEAD_DIM), C ** -0.5, 0.5, ((1, 2),))
    w_bias = centred(streams_of[8], (C, HEADS), (C // 8) ** -0.5, 1.5, ((1, 2),))
    w_out = centred(streams_of[9], (HEADS * HEAD_DIM, C), (HEADS * HEAD_DIM // 16) ** -0.5, 2.0)
    return dict(pair=pair, seq_length=seq_length, tile_counts=tile_counts, ln_gain=ln_gain, w_query=w_query, w_key=w_key, w_value=w_value, w_gate=w_gate, w_bias=w_bias, w_out=w_out)


norm_epsilon = 1e-05
masked_score = -1e+30

def layer_norm(values, gain):
    center = values - lax.optimization_barrier(jnp.mean(values, axis=-1, keepdims=True))
    spread = lax.optimization_barrier(jnp.mean(center * center, axis=-1, keepdims=True))
    return center * lax.rsqrt(spread + norm_epsilon) * gain

def reference(pair, seq_length, tile_counts, ln_gain, w_query, w_key, w_value, w_gate, w_bias, w_out):
    width = HEADS * HEAD_DIM
    normed = layer_norm(pair.astype(jnp.float32), ln_gain).astype(jnp.bfloat16)
    flat = normed.reshape(L * L, C)
    queries = (jnp.dot(flat, w_query, preferred_element_type=jnp.float32) * HEAD_DIM ** (-0.5)).astype(jnp.bfloat16).reshape(L, L, HEADS, HEAD_DIM)
    keys_all = jnp.dot(flat, w_key, preferred_element_type=jnp.float32).astype(jnp.bfloat16).reshape(L, L, HEADS, HEAD_DIM)
    values_all = jnp.dot(flat, w_value, preferred_element_type=jnp.float32).astype(jnp.bfloat16).reshape(L, L, HEADS, HEAD_DIM)
    gate_act = jax.nn.sigmoid(jnp.dot(flat, w_gate, preferred_element_type=jnp.float32)).reshape(L, L, width)
    pair_bias = jnp.einsum('jkc,ch->hjk', normed.astype(jnp.float32), w_bias.astype(jnp.float32))
    positions = jnp.arange(L, dtype=jnp.int32)
    allowed = (positions[None, :] < seq_length[0]) & ((positions % TILE)[None, :] < jnp.repeat(tile_counts, TILE, axis=1))

    def one_row(operands):
        row_queries, row_keys, row_values, row_allowed = operands
        shown = row_allowed[None, None, :]
        scores = jnp.einsum('jhd,khd->hjk', row_queries.astype(jnp.float32), row_keys.astype(jnp.float32)) + pair_bias
        scores = jnp.where(shown, scores, masked_score)
        row_max = lax.optimization_barrier(jnp.max(scores, axis=-1, keepdims=True))
        weights = jnp.where(shown, jnp.exp(scores - row_max), 0.0)
        row_sum = lax.optimization_barrier(jnp.sum(weights, axis=-1))
        rounded = lax.optimization_barrier(weights.astype(jnp.bfloat16)).astype(jnp.float32)
        mixed = jnp.einsum('hjk,khd->jhd', rounded, row_values.astype(jnp.float32))
        denom = jnp.maximum(row_sum, 1.0)
        return (mixed / jnp.transpose(denom)[:, :, None]).astype(jnp.bfloat16)
    attended = lax.map(one_row, (queries, keys_all, values_all, allowed))
    attended = lax.optimization_barrier(attended.reshape(L, L, width)).astype(jnp.float32)
    gated = (gate_act * attended).astype(jnp.bfloat16)
    update = jnp.dot(gated.reshape(L * L, width), w_out, preferred_element_type=jnp.float32)
    return update.astype(jnp.bfloat16).reshape(L, L, C)
```

```python
import functools

import jax
import jax.numpy as jnp
from jax import lax
from jax.experimental import pallas as pl
from jax.experimental.pallas import tpu as pltpu
from jax.sharding import PartitionSpec as P

HEAD_DIM = 32
TILE = 128
QUERY_TILE = 512
UNROLL = 1

norm_epsilon = 1e-05
masked_score = -1e30


def layer_norm(values, gain):
    center = values - jnp.mean(values, axis=-1, keepdims=True)
    spread = jnp.mean(center * center, axis=-1, keepdims=True)
    return center * lax.rsqrt(spread + norm_epsilon) * gain


def dot_nt(a, b):
    return lax.dot_general(a, b, (((1,), (1,)), ((), ())), preferred_element_type=jnp.float32)


def bias_kernel(_, pair_ref, gain_ref, w_ref, out_ref):
    rows, cols, channels = pair_ref.shape
    flat = pair_ref[...].reshape(rows * cols, channels).astype(jnp.float32)
    normed = layer_norm(flat, gain_ref[...]).astype(jnp.bfloat16)
    out_ref[...] = dot_nt(w_ref[...], normed).astype(jnp.bfloat16)


def pair_bias_part(pair, share, rows, gain, w_bias_t):
    _, cols, channels = pair.shape
    heads_pad = w_bias_t.shape[0]
    block = min(rows, 8)
    steps = rows // block
    return pl.pallas_call(
        bias_kernel,
        grid_spec=pltpu.PrefetchScalarGridSpec(
            num_scalar_prefetch=1,
            grid=(steps,),
            in_specs=[
                pl.BlockSpec((block, cols, channels), lambda r, which: (which[0] * steps + r, 0, 0)),
                pl.BlockSpec((1, channels), lambda r, which: (0, 0)),
                pl.BlockSpec((heads_pad, channels), lambda r, which: (0, 0)),
            ],
            out_specs=pl.BlockSpec((heads_pad, block * cols), lambda r, which: (0, r)),
        ),
        out_shape=jax.ShapeDtypeStruct((heads_pad, rows * cols), jnp.bfloat16),
        cost_estimate=pl.CostEstimate(
            flops=rows * cols * channels * 40, bytes_accessed=rows * cols * channels * 2,
            transcendentals=0,
        ),
        name="pair_bias",
    )(share, pair, gain, w_bias_t)


def attention_kernel(
    seq_ref, counts_ref, pair_ref, gain_ref, w_ref, w_out_ref, bias_ref, out_ref,
    query_s, key_s, value_s, gate_s, *, row_base,
):
    parts, _, cols, channels = pair_ref.shape
    length = parts * cols
    heads = bias_ref.shape[0]
    row = row_base + pl.program_id(0)
    seq_length = seq_ref[0]

    lane = lax.broadcasted_iota(jnp.int32, (TILE, channels), 1)
    depth = lax.broadcasted_iota(jnp.int32, (TILE, channels), 0)

    @pl.when(pl.program_id(0) == 0)
    def _():
        first_lane = jnp.where(lane == 0, 1.0, 0.0).astype(jnp.bfloat16)
        for t in range(length // TILE):
            query_s[t * TILE : (t + 1) * TILE, channels:] = first_lane

    flat = pair_ref[...].reshape(length, channels).astype(jnp.float32)
    normed = layer_norm(flat, gain_ref[...]).astype(jnp.bfloat16)
    projected = jnp.dot(normed, w_ref[...], preferred_element_type=jnp.float32)
    query_s[:, :channels] = (projected[:, :channels] * HEAD_DIM ** (-0.5)).astype(jnp.bfloat16)
    gate_s[...] = jax.nn.sigmoid(projected[:, 3 * channels :])
    for t in range(length // TILE):
        span = slice(t * TILE, (t + 1) * TILE)
        limit = jnp.minimum(counts_ref[row, t], seq_length - t * TILE)
        shown = depth < limit
        hidden = jnp.where(shown, 0.0, masked_score).astype(jnp.bfloat16)
        keys = projected[span, channels : 2 * channels]
        values = projected[span, 2 * channels : 3 * channels]
        for h in range(heads):
            mine = (lane >= h * HEAD_DIM) & (lane < (h + 1) * HEAD_DIM)
            both = mine & shown
            key_s[h, span, :channels] = jnp.where(mine, keys, 0.0).astype(jnp.bfloat16)
            key_s[h, span, channels:] = hidden
            value_s[h, span, :channels] = jnp.where(both, values, 0.0).astype(jnp.bfloat16)
            value_s[h, span, channels:] = jnp.where(both, 1.0, 0.0).astype(jnp.bfloat16)

    size = min(QUERY_TILE, length)
    out_cols = out_ref.shape[2]

    def one_tile(t, carry):
        start = pl.multiple_of(t * size, size)
        span = pl.ds(start, size)
        queries = query_s[span, :]
        total = None
        for h in range(heads):
            scores = dot_nt(queries, key_s[h]) + bias_ref[h, span, :].astype(jnp.float32)
            weights = jnp.exp(scores - jnp.max(scores, axis=-1, keepdims=True))
            term = jnp.dot(
                weights.astype(jnp.bfloat16), value_s[h], preferred_element_type=jnp.float32
            )
            total = term if total is None else total + term
        attended = total[:, :channels] / jnp.maximum(total[:, channels:], 1.0)
        attended = attended.astype(jnp.bfloat16).astype(jnp.float32)
        gated = (gate_s[span, :] * attended).astype(jnp.bfloat16)
        update = jnp.dot(gated, w_out_ref[...], preferred_element_type=jnp.float32)
        update = update.astype(jnp.bfloat16)
        ratio = size // out_cols
        for d in range(ratio):
            out_ref[t * ratio + d, 0] = update[d * out_cols : (d + 1) * out_cols]
        return carry

    lax.fori_loop(0, length // size, one_tile, 0, unroll=UNROLL)


def attention(
    seq_length, counts, pair, gain, weights, w_out, bias, row_base, first, rows, shards
):
    parts, _, cols, channels = pair.shape
    length = parts * cols
    heads = bias.shape[0]
    out_cols = length // shards
    whole = lambda *shape: pl.BlockSpec(
        shape, lambda r: (0,) * len(shape), pipeline_mode=pl.Buffered(1)
    )
    smem = pl.BlockSpec(memory_space=pltpu.SMEM)
    work = rows * heads * length * length
    return pl.pallas_call(
        functools.partial(attention_kernel, row_base=row_base),
        grid=(rows,),
        in_specs=[
            smem,
            smem,
            pl.BlockSpec((parts, 1, cols, channels), lambda r: (0, first + r, 0, 0)),
            whole(1, channels),
            whole(*weights.shape),
            whole(*w_out.shape),
            whole(*bias.shape),
        ],
        out_specs=pl.BlockSpec((shards, 1, out_cols, channels), lambda r: (0, r, 0, 0)),
        out_shape=jax.ShapeDtypeStruct((shards, rows, out_cols, channels), jnp.bfloat16),
        scratch_shapes=[
            pltpu.VMEM((length, 2 * channels), jnp.bfloat16),
            pltpu.VMEM((heads, length, 2 * channels), jnp.bfloat16),
            pltpu.VMEM((heads, length, 2 * channels), jnp.bfloat16),
            pltpu.VMEM((length, channels), jnp.float32),
        ],
        cost_estimate=pl.CostEstimate(
            flops=work * 1024, bytes_accessed=rows * length * channels * 4, transcendentals=work
        ),
        name="row_attention",
    )(seq_length, counts, pair, gain, weights, w_out, bias)


def chunk_sizes(rows):
    sizes = []
    left = rows
    while left > 1 and left > rows // 8:
        take = (left * 3 + 7) // 8
        sizes.append(take)
        left -= take
    return sizes + [left] if left else sizes


def per_device(
    pair, seq_length, tile_counts, ln_gain, w_query, w_key, w_value, w_gate, w_bias, w_out
):
    rows_dev, cols_dev, channels = pair.shape
    key_groups = lax.axis_size("keys")
    head_groups = lax.axis_size("heads")
    shards = key_groups * head_groups
    rows = rows_dev // shards
    heads_dev = w_bias.shape[1]
    heads = heads_dev * head_groups
    length = cols_dev * key_groups
    head_rank = lax.axis_index("heads")
    my_shard = lax.axis_index("keys") * head_groups + head_rank
    gain = ln_gain.reshape(1, channels)

    by_owner = pair.reshape(key_groups, head_groups, rows, cols_dev, channels)
    leaving = lax.dynamic_index_in_dim(by_owner, head_rank, 1, keepdims=False)
    arrived = lax.all_to_all(leaving, "keys", split_axis=0, concat_axis=0, tiled=True)
    counts = lax.dynamic_slice_in_dim(tile_counts, my_shard * rows, rows, 0)

    local = jnp.concatenate([w_query, w_key, w_value, w_gate, w_bias], axis=1)
    gathered = lax.all_gather(local, "heads", axis=0)
    width = w_query.shape[1]
    big = gathered[:, :, : 4 * width].reshape(head_groups, channels, 4, width)
    weights = jnp.transpose(big, (1, 2, 0, 3)).reshape(channels, 4 * width * head_groups)
    bias_t = jnp.transpose(gathered[:, :, 4 * width :], (0, 2, 1)).reshape(heads, channels)
    bias_t = jnp.pad(bias_t, ((0, -heads % 16), (0, 0)))

    share = rows_dev // head_groups
    rank = jnp.reshape(head_rank, (1,)).astype(jnp.int32)
    part = pair_bias_part(pair, rank, share, gain, bias_t)[:heads].reshape(heads, share, cols_dev)
    everyone = lax.all_gather(part, ("rows", "keys", "heads"), axis=0)
    everyone = everyone.reshape(-1, key_groups, head_groups, heads, share, cols_dev)
    bias = jnp.transpose(everyone, (3, 0, 2, 4, 1, 5)).reshape(heads, length, length)

    pieces = []
    done = 0
    for part in chunk_sizes(rows):
        update = attention(
            seq_length, counts, arrived, gain, weights, w_out, bias,
            done, done, part, shards,
        )
        done += part
        pieces.append(
            lax.all_to_all(update, ("keys", "heads"), split_axis=0, concat_axis=0, tiled=True)
        )
    return jnp.concatenate(pieces, axis=1).reshape(rows_dev, length // shards, channels)


def solution(mesh):
    in_specs = (
        P(("groups", "rows"), "keys", None),
        P("groups"),
        P(("groups", "rows"), None),
        P(),
        P(None, "heads"),
        P(None, "heads"),
        P(None, "heads"),
        P(None, "heads"),
        P(None, "heads"),
        P(),
    )
    out_specs = P(("groups", "rows"), ("keys", "heads"), None)
    return jax.shard_map(
        per_device, mesh=mesh, in_specs=in_specs, out_specs=out_specs, check_vma=False
    )
```
